32 devices in a mesh: grp: 8 (over y, x, core), blk: 4 (over z).
Axes of the slice: x: 2, y: 2, z: 4, core: 2. Of those that a mesh axis runs over, the one named last changes fastest.
Arguments:
- tokens: bfloat16 [256, 6144], P(('grp', 'blk')), may hold values from -6 to 6
- norm_gain: bfloat16 [6144], replicated, may hold values from 0.099609375 to 1.8984375
- expert_ids: int32 [256, 2], P(('grp', 'blk')), may hold values from 0 to 7, all different within a row; in each aligned block of 8 rows (0 to 7, 8 to 15, ...) at most 3 rows name the same one
- combine: float32 [256, 2], P(('grp', 'blk')), may hold values from 0.2 to 1
- w_gate: bfloat16 [6144, 65536], P(None, ('grp', 'blk')), may hold values from -0.078125 to 0.078125
- w_up: bfloat16 [6144, 65536], P(None, ('grp', 'blk')), may hold values from -0.078125 to 0.078125
- w_down: bfloat16 [65536, 6144], P(('grp', 'blk')), may hold values from -0.0625 to 0.0625
Outputs:
- layer_out: bfloat16 [256, 6144], P(('grp', 'blk'))
The draws below stay inside these ranges and needn't reach their ends.
Inputs may be any that keep to these rules, and one draw needn't show every extreme that they name: `expert_ids`: each row names 2 different experts; in the rows of one device no expert is named more than 3 times, a bound that some block reaches.
All inputs are finite; a program needn't handle non-finite values.
Results may differ from the reference program's by a relative error of at most 0.0075.
Values may be sent and summed in bfloat16 or wider, within the bound.
No kernel may reach another device: no remote copies, remote signals or barrier semaphores. Data moves between devices by JAX's collectives and lax.ppermute only.
A program may use at most 128 MiB of HBM per device.

```python
import math
import jax
import jax.numpy as jnp
import numpy as np
from jax import lax

D = 6144
FF = 8192
E = 8
TOP = 2
TOK_DEV = 8
CAP = 3
TOKENS = 256
N_GRP = 8
N_BLK = 4


def steps_of(stream_key, shape, shards, smallest, largest):
    def one(axis_at, shards_of):
        steps = jax.random.uniform(jax.random.fold_in(jax.random.fold_in(stream_key, 6), axis_at), (shards_of,), jnp.float32, smallest / len(shards), largest / len(shards))
        return jnp.repeat(jnp.exp(steps), shape[axis_at] // shards_of).reshape((-1,) + (1,) * (len(shape) - axis_at - 1))

    loudness = one(*shards[0])
    for cut in shards[1:]:
        loudness = loudness * one(*cut)
    return loudness


def routed_block(rng, own, number, rows, number_of, top, reach, skew):
    ranking = jax.random.permutation(rng, number_of)
    packed, usual = shares(number_of, rows * top, reach, skew, True), shares(number_of, rows * top, reach, skew, False)
    places = jnp.arange(number_of)

    def named(lengths, turn):
        used = int((lengths > 0).sum())
        fixed = max(1, used // 4)
        passed = fixed + (places - fixed + turn * (used - fixed)) % max(1, number_of - fixed)
        return jnp.zeros((number_of,), jnp.int32).at[ranking[jnp.where(places < fixed, places, passed)]].set(jnp.asarray(lengths, jnp.int32))

    lengths = jnp.where(number % 4 == 0, named(packed, number // 4), named(usual, number - number // 4 - 1))
    mixed = jax.random.permutation(jax.random.fold_in(own, 3), number_of)
    source_of, receiver = mixed[0:number_of // 2 * 2:2], mixed[1:number_of // 2 * 2:2]
    margin = jnp.minimum(lengths[source_of] - 1, reach - lengths[receiver]) // 2
    margin = jnp.where((source_of == ranking[0]) | (receiver == ranking[0]) | (lengths[receiver] == 0), 0, jnp.maximum(margin, 0))
    passed = jax.random.randint(jax.random.fold_in(own, 4), (number_of // 2,), 0, 1 << 20) % (margin + 1)
    lengths = lengths.at[source_of].add(-passed).at[receiver].add(passed)
    items = jnp.searchsorted(jnp.cumsum(lengths), jnp.arange(rows * top), side="right").astype(jnp.int32)
    listing = items.reshape(top, rows).T
    listing = listing[jax.random.permutation(jax.random.fold_in(own, 1), rows)]
    turn = jax.random.randint(jax.random.fold_in(own, 2), (rows, 1), 0, top)
    return jnp.take_along_axis(listing, (jnp.arange(top)[None, :] + turn) % top, axis=1)


def shares(amount, total, reach, lean, full):
    portions = [(1 << 20) // math.isqrt(rank ** lean) + 1 for rank in range(1, amount + 1)]
    largest = reach if full else min(reach, max(-(-total // amount), total * portions[0] // sum(portions)))
    least = 1 if total - largest >= amount - 1 else 0
    counts, rest = [largest] + [least] * (amount - 1), total - largest - least * (amount - 1)
    while rest > 0:
        candidates = [i for i in range(1, amount) if counts[i] < largest] or [i for i in range(1, amount) if counts[i] < reach]
        whole, left = sum([portions[i] for i in candidates]), rest
        for i in candidates:
            extra = min(reach - counts[i], max(1, left * portions[i] // whole), rest)
            counts[i] = counts[i] + extra
            rest = rest - extra
    return np.array(counts)


def gaussian(rng, shape, width, bound, split=(), kind=jnp.bfloat16):
    factor_of = steps_of(rng, shape, split, -0.22, 0.18) if split else 1.0
    entries = jax.random.normal(rng, shape, jnp.float32) * width * factor_of
    return jnp.minimum(jnp.maximum(entries, -bound), bound).astype(kind)


def setup_inputs(seed: int = 0) -> dict:
    keys = jax.random.split(jax.random.key(seed), 8)
    tokens = gaussian(keys[0], (TOKENS, D), 1.0, 6.0, ((0, 32),))
    norm_gain = jnp.clip(1.0 + 0.18 * jax.random.normal(keys[1], (D,), jnp.float32), 0.099609375, 1.8984375).astype(jnp.bfloat16)
    expert_ids_keys = jax.random.split(jax.random.fold_in(keys[2], 1), TOKENS // TOK_DEV)
    expert_ids_turns = jax.random.permutation(jax.random.fold_in(keys[2], 3), TOKENS // TOK_DEV)
    expert_ids = jax.vmap(lambda own, number: routed_block(jax.random.fold_in(keys[2], 2), own, number, TOK_DEV, E, TOP, CAP, 2))(expert_ids_keys, expert_ids_turns).reshape((TOKENS, TOP))
    combine = jnp.clip(jnp.exp(math.log(1.0) - 1.609438 * jax.random.uniform(keys[3], (TOKENS, TOP), jnp.float32) ** steps_of(keys[3], (TOKENS, TOP), ((0, 32),), -0.2, 0.2)), 0.2, 1.0)
    w_gate = gaussian(keys[4], (D, E * FF), D ** -0.5, 0.078125, ((1, 32),))
    w_up = gaussian(keys[5], (D, E * FF), D ** -0.5, 0.078125, ((1, 32),))
    w_down = gaussian(keys[6], (E * FF, D), FF ** -0.5, 0.0625, ((0, 32),))
    return {"tokens": tokens, "norm_gain": norm_gain, "expert_ids": expert_ids, "combine": combine, "w_gate": w_gate, "w_up": w_up, "w_down": w_down}


epsilon = 1e-05

def reference(tokens, norm_gain, expert_ids, combine, w_gate, w_up, w_down):
    blocks = TOKENS // TOK_DEV
    pair_count = TOKENS * TOP
    per_block = TOK_DEV * TOP
    wide_tokens = tokens.astype(jnp.float32)
    scale_rows = lax.rsqrt(lax.optimization_barrier(jnp.mean(wide_tokens * wide_tokens, axis=1, keepdims=True)) + epsilon)
    normed = (wide_tokens * scale_rows * norm_gain.astype(jnp.float32)[None, :]).astype(jnp.bfloat16)
    pair_rows = jnp.repeat(normed, TOP, axis=0)
    block_ids = expert_ids.reshape(blocks, per_block)
    one_hot = (block_ids[:, :, None] == jnp.arange(E, dtype=jnp.int32)[None, None, :]).astype(jnp.int32)
    earlier = jnp.cumsum(one_hot, axis=1) - one_hot
    slot_index = lax.optimization_barrier(jnp.sum(earlier * one_hot, axis=2))
    global_slot = (slot_index + CAP * jnp.arange(blocks, dtype=jnp.int32)[:, None]).reshape(pair_count).astype(jnp.int32)
    route_ids = expert_ids.reshape(pair_count).astype(jnp.int32)
    slot_table = jnp.zeros((E, blocks * CAP), jnp.int32).at[route_ids, global_slot].set(jnp.arange(pair_count, dtype=jnp.int32))
    unit_count = E * FF // (N_GRP * N_BLK)

    def one_expert(expert_index):
        chosen = pair_rows[slot_table[expert_index]]
        gate_cols = lax.dynamic_slice_in_dim(w_gate, expert_index * FF, FF, 1)
        up_cols = lax.dynamic_slice_in_dim(w_up, expert_index * FF, FF, 1)
        down_rows = lax.dynamic_slice_in_dim(w_down, expert_index * FF, FF, 0)
        gate_val = jnp.dot(chosen, gate_cols, preferred_element_type=jnp.float32)
        up_val = jnp.dot(chosen, up_cols, preferred_element_type=jnp.float32)
        hidden = (jax.nn.silu(gate_val) * up_val).astype(jnp.bfloat16)

        def add_block(block_index, running):
            start = (block_index * unit_count).astype(jnp.int32)
            partial_value = jnp.dot(lax.dynamic_slice_in_dim(hidden, start, unit_count, 1), lax.dynamic_slice_in_dim(down_rows, start, unit_count, 0), preferred_element_type=jnp.float32)
            rounded = lax.optimization_barrier(partial_value.astype(jnp.bfloat16))
            return running + rounded.astype(jnp.float32)
        return lax.fori_loop(0, FF // unit_count, add_block, jnp.zeros((blocks * CAP, D), jnp.float32))
    outputs = lax.map(one_expert, jnp.arange(E, dtype=jnp.int32))
    pair_out = outputs[route_ids, global_slot]
    expert_mix = lax.optimization_barrier(jnp.sum(pair_out.reshape(TOKENS, TOP, D) * combine[:, :, None], axis=1))
    return (wide_tokens + expert_mix).astype(jnp.bfloat16)
```

```python
import functools

import jax
import jax.numpy as jnp
from jax import lax
from jax.experimental import pallas as pl
from jax.experimental.pallas import tpu as pltpu
from jax.sharding import PartitionSpec as P

E = 8
TOP = 2
CAP = 3
LANES = 128

epsilon = 1e-05


def ffn_kernel(
    bk, bn, x_ref, wg_ref, wu_ref, wd_ref, o_ref, gbuf, ubuf, dbuf, gacc, uacc, hid, gsem, usem, dsem
):
    slots = gbuf.shape[0]
    k_steps = x_ref.shape[1] // bk
    n_steps = o_ref.shape[1] // bn
    per_step = -(-n_steps // slots)

    def gate_copy(i, s):
        return pltpu.make_async_copy(wg_ref.at[pl.ds(i * bk, bk), :], gbuf.at[s], gsem.at[s])

    def up_copy(i, s):
        return pltpu.make_async_copy(wu_ref.at[pl.ds(i * bk, bk), :], ubuf.at[s], usem.at[s])

    def down_copy(j):
        return pltpu.make_async_copy(wd_ref.at[:, pl.ds(j * bn, bn)], dbuf.at[j], dsem.at[j])

    for s in range(slots):
        gate_copy(s, s).start()
        up_copy(s, s).start()
    gacc[...] = jnp.zeros_like(gacc)
    uacc[...] = jnp.zeros_like(uacc)

    def step(i, carry):
        s = lax.rem(i, slots)
        x = x_ref[:, pl.ds(pl.multiple_of(i * bk, bk), bk)]
        gate_copy(i, s).wait()
        gacc[...] += jnp.dot(x, gbuf[s], preferred_element_type=jnp.float32)
        up_copy(i, s).wait()
        uacc[...] += jnp.dot(x, ubuf[s], preferred_element_type=jnp.float32)

        @pl.when(i + slots < k_steps)
        def _():
            gate_copy(i + slots, s).start()
            up_copy(i + slots, s).start()

        for q in range(per_step):
            j = (i - (k_steps - slots)) * per_step + q

            @pl.when((i + slots >= k_steps) & (j < n_steps))
            def _():
                down_copy(j).start()

        return carry

    lax.fori_loop(0, k_steps, step, 0)
    gate = gacc[...]
    hid[...] = (gate / (1.0 + jnp.exp(-gate)) * uacc[...]).astype(hid.dtype)

    def down_step(j, carry):
        down_copy(j).wait()
        o_ref[:, pl.ds(pl.multiple_of(j * bn, bn), bn)] = jnp.dot(
            hid[...], dbuf[j], preferred_element_type=jnp.float32
        ).astype(o_ref.dtype)
        return carry

    lax.fori_loop(0, n_steps, down_step, 0)


def ffn(x, w_gate, w_up, w_down):
    rows, width = x.shape
    units = w_gate.shape[1]
    bk = bn = 512
    slots = 5
    vmem = pl.BlockSpec(memory_space=pltpu.VMEM)
    hbm = pl.BlockSpec(memory_space=pl.ANY)
    return pl.pallas_call(
        functools.partial(ffn_kernel, bk, bn),
        out_shape=jax.ShapeDtypeStruct((rows, width), jnp.bfloat16),
        in_specs=[vmem, hbm, hbm, hbm],
        out_specs=vmem,
        scratch_shapes=[
            pltpu.VMEM((slots, bk, units), jnp.bfloat16),
            pltpu.VMEM((slots, bk, units), jnp.bfloat16),
            pltpu.VMEM((width // bn, units, bn), jnp.bfloat16),
            pltpu.VMEM((rows, units), jnp.float32),
            pltpu.VMEM((rows, units), jnp.float32),
            pltpu.VMEM((rows, units), jnp.bfloat16),
            pltpu.SemaphoreType.DMA((slots,)),
            pltpu.SemaphoreType.DMA((slots,)),
            pltpu.SemaphoreType.DMA((width // bn,)),
        ],
        compiler_params=pltpu.CompilerParams(vmem_limit_bytes=58 * 2**20),
        cost_estimate=pl.CostEstimate(
            flops=6 * rows * width * units, bytes_accessed=6 * width * units, transcendentals=0
        ),
        name="ffn",
    )(x, w_gate, w_up, w_down)


def split3(value):
    high = lax.reduce_precision(value, 8, 7)
    rest = value - high
    mid = lax.reduce_precision(rest, 8, 7)
    low = lax.reduce_precision(rest - mid, 8, 7)
    return [part.astype(jnp.bfloat16) for part in (high, mid, low)]


def swap(rows, groups, count):
    blocks = rows.reshape(groups, count, rows.shape[1])
    got = [blocks[0]]
    for s in range(1, groups):
        got.append(lax.ppermute(blocks[s], "grp", [(i, i ^ s) for i in range(groups)]))
    return jnp.stack(got, axis=0).reshape(rows.shape)


def on_device(tokens, norm_gain, expert_ids, combine, w_gate, w_up, w_down):
    group_count = lax.axis_size("grp")
    line = lax.axis_size("blk")
    per_group = group_count // E
    tok_count, model_width = tokens.shape
    wide_tokens = tokens.astype(jnp.float32)
    scale_rows = lax.rsqrt(jnp.mean(wide_tokens * wide_tokens, axis=1, keepdims=True) + epsilon)
    normed = (wide_tokens * scale_rows * norm_gain.astype(jnp.float32)[None, :]).astype(
        jnp.bfloat16
    )
    facts = jnp.concatenate([expert_ids.astype(jnp.bfloat16)] + split3(combine), axis=1)
    facts = jnp.pad(facts, ((0, 0), (0, LANES - facts.shape[1])))
    packed = jnp.concatenate([normed, facts], axis=1)
    parts = [packed]
    for shift in range(1, line):
        ring = [(i, (i + shift) % line) for i in range(line)]
        parts.append(lax.ppermute(packed, "blk", ring))
    gathered = jnp.concatenate(parts, axis=0)
    line_tokens = gathered[:, :model_width]
    line_facts = gathered[:, model_width:]
    count = line * tok_count
    ids = line_facts[:, :TOP].astype(jnp.float32).astype(jnp.int32)
    weight_parts = [line_facts[:, TOP * (1 + n) : TOP * (2 + n)] for n in range(3)]

    experts = jnp.arange(E, dtype=jnp.int32)
    choice = ids[:, :, None] == experts[None, None, :]
    named = jnp.any(choice, axis=1)
    place = jnp.arange(count, dtype=jnp.int32)
    before = (place[:, None] > place[None, :]) & (
        place[:, None] // tok_count == place[None, :] // tok_count
    )
    earlier = jnp.sum((before[:, :, None] & named[None, :, :]).astype(jnp.int32), axis=1)
    rows = group_count * line * CAP
    row = jnp.arange(rows, dtype=jnp.int32)
    me = lax.axis_index("grp")
    row_expert = (me ^ (row // (line * CAP))) // per_group
    row_block = row // CAP % line
    row_slot = row % CAP
    row_is = row_expert[:, None] == experts[None, :]
    pick = jnp.sum(jnp.where(row_is[:, None, :] & named[None, :, :], earlier[None, :, :] + 1, 0), axis=2)
    hit = (pick == row_slot[:, None] + 1) & (row_block[:, None] == place[None, :] // tok_count)
    placer = hit.astype(jnp.bfloat16)
    outgoing = jnp.dot(placer, line_tokens, preferred_element_type=jnp.float32).astype(jnp.bfloat16)
    arrived = swap(outgoing, group_count, line * CAP)
    partial_rows = ffn(arrived, w_gate, w_up, w_down)
    returned = swap(partial_rows, group_count, line * CAP)
    mixers = []
    for weights in weight_parts:
        per_expert = jnp.sum(jnp.where(choice, weights.astype(jnp.float32)[:, :, None], 0.0), axis=1)
        per_row = jnp.sum(jnp.where(row_is[None, :, :], per_expert[:, None, :], 0.0), axis=2)
        mixers.append(jnp.where(hit.T, per_row, 0.0).astype(jnp.bfloat16))
    mixer = jnp.concatenate(mixers, axis=0)
    mixed = jnp.dot(mixer, returned, preferred_element_type=jnp.float32)
    mixed = jnp.sum(mixed.reshape(3, line, tok_count, model_width), axis=0)
    total = wide_tokens + mixed[0]
    for shift in range(1, line):
        ring = [((i + shift) % line, i) for i in range(line)]
        total = total + lax.ppermute(mixed[shift].astype(jnp.bfloat16), "blk", ring).astype(jnp.float32)
    return total.astype(jnp.bfloat16)


def solution(mesh):
    return jax.shard_map(
        on_device,
        mesh=mesh,
        in_specs=(
            P(("grp", "blk"), None),
            P(),
            P(("grp", "blk"), None),
            P(("grp", "blk"), None),
            P(None, ("grp", "blk")),
            P(None, ("grp", "blk")),
            P(("grp", "blk"), None),
        ),
        out_specs=P(("grp", "blk"), None),
        check_vma=False,
    )
```
